256 devices in a mesh: segment: 8 (over x, y_hi), dp: 32 (over y_lo, z, core).
Axes of the slice: x: 4, y: 4 (y_hi: 2, y_lo: 2; y = y_hi * 2 + y_lo), z: 8, core: 2. Of those that a mesh axis runs over, the one named last changes fastest.
Arguments:
- encoder_patch_input: bfloat16 [32, 1024, 1024], P('dp'), may hold values from -6 to 6
- encoder_norm_gains: float32 [8, 1024], P('segment'), may hold values from 0.5 to 1.5
- encoder_input_weight: bfloat16 [8, 1024, 2048], P('segment'), may hold values from -0.1875 to 0.1875
- encoder_output_weight: bfloat16 [8, 2048, 1024], P('segment'), may hold values from -0.125 to 0.125
- diffuser_hidden_states: bfloat16 [32, 1024, 2048], P('dp', 'segment'), may hold values from -6 to 6
- projector_first_weight: bfloat16 [2048, 2048], P('dp', 'segment'), may hold values from -0.125 to 0.125
- projector_second_weight: bfloat16 [2048, 1024], P(('segment', 'dp')), may hold values from -0.125 to 0.125
Outputs:
- grad_w1: float32 [2048, 2048], P('dp', 'segment')
- grad_w2: float32 [2048, 1024], P(('segment', 'dp'))
The draws below stay inside these ranges and needn't reach their ends.
All inputs are finite; a program needn't handle non-finite values.
Results may differ from the reference program's by a relative error of at most 0.014.
Values may be sent and summed in bfloat16 or wider, within the bound.
A program may use at most 128 MiB of HBM per device.

```python
import jax
import jax.numpy as jnp
from jax import lax

ENCODER_WIDTH = 1024
EFF = 2048
DIFFUSER_WIDTH = 2048
HALF_PROJ_UNITS = 2048
LAYERS = 8
RECORDING_SETS = 32
SET_TOKENS = 1024


def steps_of(stream_key, extent, pieces, low, largest):
    loudness, own = 1.0, jax.random.fold_in(stream_key, 6)
    for position, blocks in pieces:
        draws = jnp.exp(jax.random.uniform(jax.random.fold_in(own, position), (blocks,), jnp.float32, low / len(pieces), largest / len(pieces)))
        loudness = loudness * jnp.repeat(draws, extent[position] // blocks).reshape([-1 if axis == position else 1 for axis in range(len(extent))])
    return loudness


def normal_values(stream_key, extent, width, most, split=(), dtype=jnp.bfloat16):
    array = width * jax.random.normal(stream_key, extent, jnp.float32)
    if split:
        array = array * steps_of(stream_key, extent, split, -0.22, 0.18)
    return jnp.clip(array, -most, most).astype(dtype)


def setup_inputs(seed: int = 0) -> dict:
    arg_keys = jax.random.split(jax.random.key(seed), 8)
    return {
        "encoder_patch_input": normal_values(arg_keys[0], (RECORDING_SETS, SET_TOKENS, ENCODER_WIDTH), 1.0, 6.0, ((0, 32),)),
        "encoder_norm_gains": jnp.clip(0.5 + 1.0 * jax.random.uniform(arg_keys[1], (LAYERS, ENCODER_WIDTH), jnp.float32) ** steps_of(arg_keys[1], (LAYERS, ENCODER_WIDTH), ((0, 8),), -0.2, 0.2), 0.5, 1.5),
        "encoder_input_weight": normal_values(arg_keys[2], (LAYERS, ENCODER_WIDTH, EFF), ENCODER_WIDTH ** -0.5, 0.1875, ((0, 8),)),
        "encoder_output_weight": normal_values(arg_keys[3], (LAYERS, EFF, ENCODER_WIDTH), EFF ** -0.5, 0.125, ((0, 8),)),
        "diffuser_hidden_states": normal_values(arg_keys[4], (RECORDING_SETS, SET_TOKENS, DIFFUSER_WIDTH), 1.0, 6.0, ((0, 32), (1, 8))),
        "projector_first_weight": normal_values(arg_keys[5], (DIFFUSER_WIDTH, HALF_PROJ_UNITS), DIFFUSER_WIDTH ** -0.5, 0.125, ((0, 32), (1, 8))),
        "projector_second_weight": normal_values(arg_keys[6], (HALF_PROJ_UNITS, ENCODER_WIDTH), HALF_PROJ_UNITS ** -0.5, 0.125, ((0, 256),)),
    }


norm_eps = 1e-06

def encoder_layer(hidden, scale_row, weight_in, weight_out):
    floats = hidden.astype(jnp.float32)
    normed = floats * lax.rsqrt(lax.optimization_barrier(jnp.mean(floats * floats, axis=-1, keepdims=True)) + norm_eps) * scale_row
    inner = jnp.dot(normed.astype(jnp.bfloat16), weight_in, preferred_element_type=jnp.float32)
    inner = jax.nn.gelu(inner, approximate=True).astype(jnp.bfloat16)
    return (floats + jnp.dot(inner, weight_out, preferred_element_type=jnp.float32)).astype(jnp.bfloat16)

def cosine_grad(projected, features):
    feat_f = features.astype(jnp.float32)
    squared = lax.optimization_barrier(jnp.sum(projected * projected, axis=-1, keepdims=True)) + norm_eps
    inv_proj = lax.rsqrt(squared)
    unit_feat = feat_f * lax.rsqrt(lax.optimization_barrier(jnp.sum(feat_f * feat_f, axis=-1, keepdims=True)) + norm_eps)
    cosine = lax.optimization_barrier(jnp.sum(projected * unit_feat, axis=-1, keepdims=True)) * inv_proj
    return (cosine * projected / squared - unit_feat * inv_proj).astype(jnp.bfloat16)

def silu_slope(preact):
    sigma = jax.nn.sigmoid(preact)
    return sigma * (1.0 + preact * (1.0 - sigma))

def contract_rows(left, right):
    return lax.dot_general(left, right, (((0,), (0,)), ((), ())), preferred_element_type=jnp.float32)

def reference(encoder_patch_input, encoder_norm_gains, encoder_input_weight, encoder_output_weight, diffuser_hidden_states, projector_first_weight, projector_second_weight):

    def single_recording_set(totals, pair):
        source, hidden_rows = pair
        feats = source
        for layer in range(LAYERS):
            feats = encoder_layer(feats, encoder_norm_gains[layer], encoder_input_weight[layer], encoder_output_weight[layer])
        preact = jnp.dot(hidden_rows, projector_first_weight, preferred_element_type=jnp.float32)
        activated = jax.nn.silu(preact).astype(jnp.bfloat16)
        projected = jnp.dot(activated, projector_second_weight, preferred_element_type=jnp.float32)
        grad_proj = cosine_grad(projected, feats)
        grad_second = contract_rows(activated, grad_proj)
        back = lax.dot_general(grad_proj, projector_second_weight, (((1,), (1,)), ((), ())), preferred_element_type=jnp.float32)
        grad_pre = (back * silu_slope(preact)).astype(jnp.bfloat16)
        grad_first = contract_rows(hidden_rows, grad_pre)
        return ((totals[0] + grad_first, totals[1] + grad_second), None)
    offset_begin = (jnp.zeros((DIFFUSER_WIDTH, HALF_PROJ_UNITS), jnp.float32), jnp.zeros((HALF_PROJ_UNITS, ENCODER_WIDTH), jnp.float32))
    running_sums, ignored_value = lax.scan(single_recording_set, offset_begin, (encoder_patch_input, diffuser_hidden_states))
    return (running_sums[0], running_sums[1])
```

```python
import functools

import jax
import jax.numpy as jnp
from jax import lax
from jax.experimental import pallas as pl
from jax.experimental.pallas import tpu as pltpu
from jax.sharding import PartitionSpec as P

EPS = 1e-06
GELU_C = 0.7978845608
F32 = jnp.float32
BF16 = jnp.bfloat16
CHUNKS = 8


def gelu(v):
    return 0.5 * v * (1.0 + jnp.tanh(GELU_C * (v + 0.044715 * (v * v * v))))


def mega(
    X,
    Z,
    x0_in,
    gain_in,
    wi_in,
    wo_in,
    hid_in,
    w1_in,
    w2_in,
    g1_out,
    g2_out,
    WI,
    WO,
    gains,
    x0,
    inbox,
    outbox,
    feat,
    hid,
    W1,
    W2,
    pre,
    act,
    pbuf,
    pown,
    precv,
    gall,
    gp,
    PB,
    crecv,
    S,
    urecv,
    usend,
    drecv,
    dsend,
    rsend,
    rown,
    yrecv,
    lsem,
    gsem,
    ws,
    wr,
    hs,
    hr,
    ags,
    agr,
    pxs,
    pxr,
    pis,
    pir,
    fs,
    fr,
    pps,
    ppr,
    ggs,
    ggr,
    ccs,
    ccr,
    us,
    ur,
    ds_,
    dr,
    ys,
    yr,
):
    seg = lax.axis_index("segment")
    dp = lax.axis_index("dp")
    x = seg // 2
    yh = seg % 2
    yl = dp // (2 * Z)
    z = (dp // 2) % Z
    c = dp % 2
    y = yh * 2 + yl
    zp = z % 2
    T, D = hid.shape[1], x0.shape[2]

    def dev(xx=x, yy=y, zz=z, cc=c):
        return {
            "segment": xx * 2 + yy // 2,
            "dp": (yy % 2) * (2 * Z) + zz * 2 + cc,
        }

    def push(src, dst, ssem, rsem, to):
        pltpu.make_async_remote_copy(
            src_ref=src,
            dst_ref=dst,
            send_sem=ssem,
            recv_sem=rsem,
            device_id=to,
            device_id_type=pl.DeviceIdType.MESH,
        ).start()

    def wait(ref, sem):
        pltpu.make_async_copy(ref, ref, sem).wait()

    def loop(lo, hi, body):
        def step(i, carry):
            body(i)
            return carry

        lax.fori_loop(lo, hi, step, 0)

    partner = dev(cc=1 - c)
    cut = dev(yy=3 - y)
    mate = dev(yy=yh * 2 + (1 - yl))
    up = dev(zz=(z + 1) % Z)
    down = dev(zz=(z + Z - 1) % Z)

    local = [
        pltpu.make_async_copy(wi_in, WI.at[yh], lsem.at[0]),
        pltpu.make_async_copy(wo_in, WO.at[yh], lsem.at[1]),
        pltpu.make_async_copy(hid_in, hid.at[x], lsem.at[2]),
        pltpu.make_async_copy(gain_in, gains.at[yh], lsem.at[3]),
        pltpu.make_async_copy(
            w1_in, W1.at[yl * Z + z, c, :, pl.ds(pl.multiple_of(yh * 256, 256), 256)], lsem.at[4]
        ),
        pltpu.make_async_copy(w2_in, W2.at[yh, yl * Z + z, c], lsem.at[5]),
    ] + [
        pltpu.make_async_copy(
            x0_in.at[pl.ds(pl.multiple_of((2 * m + yh) * T, T), T), :], x0.at[m], lsem.at[6 + m]
        )
        for m in range(X)
    ]
    for copy in local:
        copy.start()

    barrier = pltpu.get_barrier_semaphore()

    def greet(to):
        pl.semaphore_signal(barrier, inc=1, device_id=to, device_id_type=pl.DeviceIdType.MESH)

    greet(partner)
    for i in range(1, X):
        greet(dev(xx=(x + i) % X))
    loop(1, 4 * Z, lambda k: greet(dev(yy=(y + k // Z) % 4, zz=(z + k % Z) % Z)))
    pl.semaphore_wait(barrier, 1 + (X - 1) + (4 * Z - 1))

    for i in range(1, X):
        push(hid_in, hid.at[x], hs.at[i], hr.at[x], dev(xx=(x + i) % X))

    push(gain_in, gains.at[yh], gsem.at[0], gsem.at[1], cut)
    other = 1 - yh

    def part(ref, slot, piece, k):
        rows = ref.shape[1] // 8
        step = rows // CHUNKS
        if slot is None:
            return ref.at[pl.ds(pl.multiple_of(piece * rows + k * step, step), step), :]
        return ref.at[slot, pl.ds(pl.multiple_of(piece * rows + k * step, step), step), :]

    def native(ref, like, piece, k):
        rows = like.shape[1] // 8
        step = rows // CHUNKS
        return ref.at[pl.ds(pl.multiple_of(piece * rows + k * step, step), step), :]

    quarter_cut = 2 * (2 * zp + (1 - yl)) + c
    quarter = [
        2 * (2 * zp + yl) + c,
        2 * (2 * zp + (1 - yl)) + c,
        2 * (2 * (1 - zp) + yl) + c,
        2 * (2 * (1 - zp) + (1 - yl)) + c,
    ]
    pair = [(0, WI, wi_in), (1, WO, wo_in)]

    def first(k):
        for w, buf, src in pair:
            push(
                native(src, buf, quarter_cut, k),
                part(buf, yh, quarter_cut, k),
                ws.at[w, 0, k],
                wr.at[w, 0, k],
                cut,
            )

    loop(0, CHUNKS, first)

    def relay(q, recv_kind, k, targets):
        for w, buf, _ in pair:
            got = part(buf, other, quarter[q], k)
            wait(got, wr.at[w, recv_kind, k])
            for kind, to in targets:
                push(got, got, ws.at[w, kind, k], wr.at[w, kind, k], to)

    def exchange(t):
        @pl.when(t < CHUNKS)
        def _():
            relay(0, 0, t, [(1, mate), (2, up), (3, partner)])

        @pl.when(jnp.logical_and(t >= 1, t < CHUNKS + 1))
        def _():
            relay(1, 1, t - 1, [(4, down), (5, partner)])

        @pl.when(jnp.logical_and(t >= 2, t < CHUNKS + 2))
        def _():
            relay(2, 2, t - 2, [(6, partner)])

        @pl.when(t >= 3)
        def _():
            relay(3, 4, t - 3, [(7, partner)])

    loop(0, CHUNKS + 3, exchange)

    mine = y * Z + z

    def gather(k):
        to = dev(yy=(y + k // Z) % 4, zz=(z + k % Z) % Z)
        push(
            w1_in,
            W1.at[yl * Z + z, c, :, pl.ds(pl.multiple_of(yh * 256, 256), 256)],
            ags.at[0, k],
            agr.at[0, mine],
            to,
        )
        push(w2_in, W2.at[yh, yl * Z + z, c], ags.at[1, k], agr.at[1, mine], to)

    loop(1, 4 * Z, gather)

    def partner_share(k):
        for q, kind in enumerate((3, 5, 6, 7)):
            for w, buf, _ in pair:
                theirs = part(buf, other, quarter[q] + (1 - 2 * c), k)
                wait(theirs, wr.at[w, kind, k])

    loop(0, CHUNKS, partner_share)
    wait(gains.at[other], gsem.at[1])
    for copy in local:
        copy.wait()

    def encode(m):
        @pl.when(x > 0)
        def _():
            wait(inbox.at[m], pir.at[m])

        @pl.when(x == 0)
        def _():
            inbox[m] = x0[m]

        def layer(j):
            h = inbox[m].astype(F32)
            scale = lax.rsqrt(jnp.mean(h * h, axis=-1, keepdims=True) + EPS)
            n = (h * scale * gains[j]).astype(BF16)
            u = jnp.dot(n, WI[j], preferred_element_type=F32)
            u = gelu(u).astype(BF16)
            r = (h + jnp.dot(u, WO[j], preferred_element_type=F32)).astype(BF16)

            @pl.when(j == 0)
            def _():
                inbox[m] = r

            @pl.when(j == 1)
            def _():
                outbox[m] = r

        loop(0, 2, layer)

        @pl.when(x < X - 1)
        def _():
            push(outbox.at[m], inbox.at[m], pis.at[m], pir.at[m], dev(xx=x + 1))

        @pl.when(jnp.logical_and(x == X - 1, m < X - 1))
        def _():
            push(outbox.at[m], feat, fs.at[m], fr, dev(xx=m))

    def project():
        def arrived(k):
            yy, zz = k // Z, k % Z
            row = (yy % 2) * Z + zz
            col = pl.multiple_of((yy // 2) * 256, 256)

            @pl.when(k != mine)
            def _():
                wait(W1.at[row, c, :, pl.ds(col, 256)], agr.at[0, k])
                wait(W2.at[yy // 2, row, c], agr.at[1, k])

        loop(0, 4 * Z, arrived)
        push(W1.at[:, c], W1.at[:, c], pxs.at[0], pxr.at[0], partner)
        for h in range(2):
            push(W2.at[h, :, c], W2.at[h, :, c], pxs.at[1 + h], pxr.at[1 + h], partner)
        for i in range(1, X):
            xx = (x + i) % X
            wait(hid.at[xx], hr.at[xx])
        wait(W1.at[:, 1 - c], pxr.at[0])
        for h in range(2):
            wait(W2.at[h, :, 1 - c], pxr.at[1 + h])

        def block(j):
            w1 = W1[...].reshape(W1.shape[0] * 2 * W1.shape[2], W1.shape[3])
            w2 = W2[...].reshape(W2.shape[0] * W2.shape[1] * 2 * W2.shape[3], W2.shape[4])
            v = jnp.dot(hid[j], w1, preferred_element_type=F32)
            pre[j] = v
            a = (v / (1.0 + jnp.exp(-v))).astype(BF16)
            act[j] = a
            p = jnp.dot(a, w2, preferred_element_type=F32)

            @pl.when(j == x)
            def _():
                pown[...] = p

            @pl.when(j != x)
            def _():
                pbuf[j] = p.astype(BF16)
                push(pbuf.at[j], precv.at[x], pps.at[j], ppr.at[x], dev(xx=j))

        loop(0, X, block)

    def order(phase):
        @pl.when((phase == 0) == (x == X - 1))
        def _():
            project()

        @pl.when(phase == 0)
        def _():
            loop(0, X, encode)

    loop(0, 2, order)

    total = pown[...]
    for i in range(1, X):
        xx = (x + i) % X
        wait(precv.at[xx], ppr.at[xx])
        total = total + precv[xx].astype(F32)

    @pl.when(x < X - 1)
    def _():
        wait(feat, fr)

    @pl.when(x == X - 1)
    def _():
        feat[...] = outbox[X - 1]

    f = feat[...].astype(F32)
    squared = jnp.sum(total * total, axis=-1, keepdims=True) + EPS
    inv = lax.rsqrt(squared)
    unit = f * lax.rsqrt(jnp.sum(f * f, axis=-1, keepdims=True) + EPS)
    cosine = jnp.sum(total * unit, axis=-1, keepdims=True) * inv
    gall[x] = (cosine * total / squared - unit * inv).astype(BF16)
    for i in range(1, X):
        push(gall.at[x], gall.at[x], ggs.at[i], ggr.at[x], dev(xx=(x + i) % X))

    def back(i):
        j = (x + i) % X

        @pl.when(i > 0)
        def _():
            wait(gall.at[j], ggr.at[j])

        w2 = W2[...].reshape(W2.shape[0] * W2.shape[1] * 2 * W2.shape[3], W2.shape[4])
        b = lax.dot_general(gall[j], w2, (((1,), (1,)), ((), ())), preferred_element_type=F32)
        v = pre[j]
        s = 1.0 / (1.0 + jnp.exp(-v))
        gp[j] = (b * (s * (1.0 + v * (1.0 - s)))).astype(BF16)

    loop(0, X, back)

    tokens = X * T
    rows_dims = (((0,), (0,)), ((), ()))
    g2 = lax.dot_general(
        act[...].reshape(tokens, act.shape[2]),
        gall[...].reshape(tokens, D),
        rows_dims,
        preferred_element_type=F32,
    ).reshape(2, 2, Z, 2, 8, D)
    gpv = gp[...].reshape(tokens, gp.shape[2])
    span = Z // 2 * 2 * 64
    for q in range(4):
        g1 = lax.dot_general(
            hid[:, :, q * span : (q + 1) * span].reshape(tokens, span),
            gpv,
            rows_dims,
            preferred_element_type=F32,
        ).reshape(Z // 2, 2, 64, 512)
        yl2, z2 = q // 2, (q % 2) * (Z // 2)
        for cc in range(2):
            for yh2 in range(2):
                PB[cc, yh2 * 2 + yl2, z2 : z2 + Z // 2, 0:64, :] = g1[
                    :, cc, :, yh2 * 256 : yh2 * 256 + 256
                ].astype(BF16)
    for cc in range(2):
        for yy in range(4):
            for zz in range(Z):
                blk = g2[yy // 2, yy % 2, zz, cc]
                PB[cc, yy, zz, 64:96, :] = jnp.concatenate(
                    [blk[:, k * 256 : k * 256 + 256] for k in range(4)], axis=0
                ).astype(BF16)

    for yy in range(4):
        push(PB.at[1 - c, yy], crecv.at[yy], ccs.at[yy], ccr.at[yy], partner)

    half = Z // 2

    def cores(yy):
        wait(crecv.at[yy], ccr.at[yy])
        S[yy] = (PB[c, yy].astype(F32) + crecv[yy].astype(F32)).astype(BF16)
        push(S.at[yy, (z + half) % Z], urecv.at[0, yy], us.at[0, yy], ur.at[0, yy], up)
        push(S.at[yy, (z + half + 1) % Z], drecv.at[0, yy], ds_.at[0, yy], dr.at[0, yy], down)

    loop(0, 4, cores)

    def ring(t):
        for yy in range(4):
            wait(urecv.at[t, yy], ur.at[t, yy])
            usend[t, yy] = (
                urecv[t, yy].astype(F32) + S[yy, (z + half - 1 - t) % Z].astype(F32)
            ).astype(BF16)
            push(usend.at[t, yy], urecv.at[t + 1, yy], us.at[t + 1, yy], ur.at[t + 1, yy], up)

            @pl.when(t < half - 2)
            def _():
                wait(drecv.at[t, yy], dr.at[t, yy])
                dsend[t, yy] = (
                    drecv[t, yy].astype(F32) + S[yy, (z + half + 2 + t) % Z].astype(F32)
                ).astype(BF16)
                push(
                    dsend.at[t, yy], drecv.at[t + 1, yy], ds_.at[t + 1, yy], dr.at[t + 1, yy], down
                )

    loop(0, half - 1, ring)

    def rows(yy):
        wait(urecv.at[half - 1, yy], ur.at[half - 1, yy])
        wait(drecv.at[half - 2, yy], dr.at[half - 2, yy])
        r = (
            S[yy, z].astype(F32)
            + urecv[half - 1, yy].astype(F32)
            + drecv[half - 2, yy].astype(F32)
        )

        @pl.when(yy == y)
        def _():
            rown[...] = r

        @pl.when(yy != y)
        def _():
            rsend[yy] = r.astype(BF16)
            push(rsend.at[yy], yrecv.at[y], ys.at[yy], yr.at[y], dev(yy=yy))

    loop(0, 4, rows)
    r = rown[...]
    for i in range(1, 4):
        yy = (y + i) % 4
        wait(yrecv.at[yy], yr.at[yy])
        r = r + yrecv[yy].astype(F32)
    g1_out[...] = r[0:64]
    for k in range(4):
        g2_out[:, k * 256 : k * 256 + 256] = r[64 + 8 * k : 72 + 8 * k]

    for i in range(1, X):
        wait(hid.at[x], hs.at[i])
        wait(gall.at[x], ggs.at[i])
    wait(gains.at[yh], gsem.at[0])

    def sent_weights(k):
        for w, buf, _ in pair:
            for kind in range(8):
                wait(part(buf, 0, 0, k), ws.at[w, kind, k])

    loop(0, CHUNKS, sent_weights)

    def sent_gather(k):
        wait(w1_in, ags.at[0, k])
        wait(w2_in, ags.at[1, k])

    loop(1, 4 * Z, sent_gather)
    wait(W1.at[:, c], pxs.at[0])
    for h in range(2):
        wait(W2.at[h, :, c], pxs.at[1 + h])

    def sent_lines(m):
        @pl.when(x < X - 1)
        def _():
            wait(outbox.at[m], pis.at[m])

        @pl.when(jnp.logical_and(x == X - 1, m < X - 1))
        def _():
            wait(outbox.at[m], fs.at[m])

        @pl.when(m != x)
        def _():
            wait(pbuf.at[m], pps.at[m])

    loop(0, X, sent_lines)

    def sent_sums(yy):
        wait(crecv.at[yy], ccs.at[yy])
        for t in range(half):
            wait(urecv.at[0, yy], us.at[t, yy])
        for t in range(half - 1):
            wait(drecv.at[0, yy], ds_.at[t, yy])

        @pl.when(yy != y)
        def _():
            wait(rsend.at[yy], ys.at[yy])

    loop(0, 4, sent_sums)


def solution(mesh):
    X = mesh.shape["segment"] // 2
    Z = mesh.shape["dp"] // 4

    def on_device(x0, gain, wi, wo, hid, w1, w2):
        x0, wi, wo, hid = x0[0], wi[0], wo[0], hid[0]
        T, W = hid.shape
        N, D = x0.shape
        E = wi.shape[1]
        H = 2 * w1.shape[1]
        half = Z // 2
        B = (96, 256)
        vm = lambda shape, dtype=BF16: pltpu.VMEM(shape, dtype)
        dma = lambda *shape: pltpu.SemaphoreType.DMA(shape)
        scratch = [
            vm((2, D, E)),
            vm((2, E, D)),
            vm((2, 1, D), F32),
            vm((X, T, D)),
            vm((X, T, D)),
            vm((X, T, D)),
            vm((T, D)),
            vm((X, T, W)),
            vm((2 * Z, 2, 64, H)),
            vm((2, 2 * Z, 2, 8, D)),
            vm((X, T, H), F32),
            vm((X, T, H)),
            vm((X, T, D)),
            vm((T, D), F32),
            vm((X, T, D)),
            vm((X, T, D)),
            vm((X, T, H)),
            vm((2, 4, Z) + B),
            vm((4, Z) + B),
            vm((4, Z) + B),
            vm((half, 4) + B),
            vm((half - 1, 4) + B),
            vm((half - 1, 4) + B),
            vm((half - 2, 4) + B),
            vm((4,) + B),
            vm(B, F32),
            vm((4,) + B),
            dma(6 + X),
            dma(2),
            dma(2, 8, CHUNKS),
            dma(2, 8, CHUNKS),
            dma(X),
            dma(X),
            dma(2, 4 * Z),
            dma(2, 4 * Z),
            dma(3),
            dma(3),
            dma(X),
            dma(X),
            dma(X),
            pltpu.SemaphoreType.DMA,
            dma(X),
            dma(X),
            dma(X),
            dma(X),
            dma(4),
            dma(4),
            dma(half, 4),
            dma(half, 4),
            dma(half - 1, 4),
            dma(half - 1, 4),
            dma(4),
            dma(4),
        ]
        any_ = pl.BlockSpec(memory_space=pl.ANY)
        vmem = pl.BlockSpec(memory_space=pltpu.VMEM)
        return pl.pallas_call(
            functools.partial(mega, X, Z),
            out_shape=(
                jax.ShapeDtypeStruct((64, 256), F32),
                jax.ShapeDtypeStruct((8, D), F32),
            ),
            in_specs=[any_, vmem, any_, any_, any_, vmem, vmem],
            out_specs=(vmem, vmem),
            scratch_shapes=scratch,
            compiler_params=pltpu.CompilerParams(
                collective_id=0, has_side_effects=True, vmem_limit_bytes=62 << 20
            ),
        )(x0, gain, wi, wo, hid, w1, w2)

    placed = (
        P("dp", None, None),
        P("segment", None),
        P("segment", None, None),
        P("segment", None, None),
        P("dp", "segment", None),
        P("dp", "segment"),
        P(("segment", "dp"), None),
    )
    return jax.shard_map(
        on_device,
        mesh=mesh,
        in_specs=placed,
        out_specs=(P("dp", "segment"), P(("segment", "dp"), None)),
        check_vma=False,
    )
```

```python
import functools

import jax
import jax.numpy as jnp
from jax import lax
from jax.experimental import pallas as pl
from jax.experimental.pallas import tpu as pltpu
from jax.sharding import PartitionSpec as P

EPS = 1e-06
GELU_C = 0.7978845608
F32 = jnp.float32
BF16 = jnp.bfloat16
CHUNKS = 8


def gelu(v):
    return 0.5 * v * (1.0 + jnp.tanh(GELU_C * (v + 0.044715 * (v * v * v))))


def mega(
    X,
    Z,
    x0_in,
    gain_in,
    wi_in,
    wo_in,
    hid_in,
    w1_in,
    w2_in,
    g1_out,
    g2_out,
    WI,
    WO,
    gains,
    x0,
    inbox,
    outbox,
    feat,
    hid,
    W1,
    W2,
    pre,
    act,
    pbuf,
    pown,
    precv,
    gall,
    gp,
    PB,
    crecv,
    S,
    urecv,
    usend,
    drecv,
    dsend,
    rsend,
    rown,
    yrecv,
    lsem,
    gsem,
    ws,
    wr,
    hs,
    hr,
    ags,
    agr,
    pxs,
    pxr,
    pis,
    pir,
    fs,
    fr,
    pps,
    ppr,
    ggs,
    ggr,
    ccs,
    ccr,
    us,
    ur,
    ds_,
    dr,
    ys,
    yr,
):
    seg = lax.axis_index("segment")
    dp = lax.axis_index("dp")
    x = seg // 2
    yh = seg % 2
    yl = dp // (2 * Z)
    z = (dp // 2) % Z
    c = dp % 2
    y = yh * 2 + yl
    zp = z % 2
    T, D = hid.shape[1], x0.shape[2]

    def dev(xx=x, yy=y, zz=z, cc=c):
        return {
            "segment": xx * 2 + yy // 2,
            "dp": (yy % 2) * (2 * Z) + zz * 2 + cc,
        }

    def push(src, dst, ssem, rsem, to):
        pltpu.make_async_remote_copy(
            src_ref=src,
            dst_ref=dst,
            send_sem=ssem,
            recv_sem=rsem,
            device_id=to,
            device_id_type=pl.DeviceIdType.MESH,
        ).start()

    def wait(ref, sem):
        pltpu.make_async_copy(ref, ref, sem).wait()

    def loop(lo, hi, body):
        def step(i, carry):
            body(i)
            return carry

        lax.fori_loop(lo, hi, step, 0)

    partner = dev(cc=1 - c)
    cut = dev(yy=3 - y)
    mate = dev(yy=yh * 2 + (1 - yl))
    up = dev(zz=(z + 1) % Z)
    down = dev(zz=(z + Z - 1) % Z)

    local = [
        pltpu.make_async_copy(wi_in, WI.at[yh], lsem.at[0]),
        pltpu.make_async_copy(wo_in, WO.at[yh], lsem.at[1]),
        pltpu.make_async_copy(hid_in, hid.at[x], lsem.at[2]),
        pltpu.make_async_copy(gain_in, gains.at[yh], lsem.at[3]),
        pltpu.make_async_copy(
            w1_in, W1.at[yl * Z + z, c, :, pl.ds(pl.multiple_of(yh * 256, 256), 256)], lsem.at[4]
        ),
        pltpu.make_async_copy(w2_in, W2.at[yh, yl * Z + z, c], lsem.at[5]),
    ] + [
        pltpu.make_async_copy(
            x0_in.at[pl.ds(pl.multiple_of((2 * m + yh) * T, T), T), :], x0.at[m], lsem.at[6 + m]
        )
        for m in range(X)
    ]
    for copy in local:
        copy.start()

    barrier = pltpu.get_barrier_semaphore()

    def greet(to):
        pl.semaphore_signal(barrier, inc=1, device_id=to, device_id_type=pl.DeviceIdType.MESH)

    greet(partner)
    for i in range(1, X):
        greet(dev(xx=(x + i) % X))
    loop(1, 4 * Z, lambda k: greet(dev(yy=(y + k // Z) % 4, zz=(z + k % Z) % Z)))
    pl.semaphore_wait(barrier, 1 + (X - 1) + (4 * Z - 1))

    for i in range(1, X):
        push(hid_in, hid.at[x], hs.at[i], hr.at[x], dev(xx=(x + i) % X))

    push(gain_in, gains.at[yh], gsem.at[0], gsem.at[1], cut)
    other = 1 - yh

    def part(ref, slot, piece, k):
        rows = ref.shape[1] // 8
        step = rows // CHUNKS
        if slot is None:
            return ref.at[pl.ds(pl.multiple_of(piece * rows + k * step, step), step), :]
        return ref.at[slot, pl.ds(pl.multiple_of(piece * rows + k * step, step), step), :]

    def native(ref, like, piece, k):
        rows = like.shape[1] // 8
        step = rows // CHUNKS
        return ref.at[pl.ds(pl.multiple_of(piece * rows + k * step, step), step), :]

    quarter_cut = 2 * (2 * zp + (1 - yl)) + c
    quarter = [
        2 * (2 * zp + yl) + c,
        2 * (2 * zp + (1 - yl)) + c,
        2 * (2 * (1 - zp) + yl) + c,
        2 * (2 * (1 - zp) + (1 - yl)) + c,
    ]
    pair = [(0, WI, wi_in), (1, WO, wo_in)]

    def first(k):
        for w, buf, src in pair:
            push(
                native(src, buf, quarter_cut, k),
                part(buf, yh, quarter_cut, k),
                ws.at[w, 0, k],
                wr.at[w, 0, k],
                cut,
            )

    mine = y * Z + z
    half = Z // 2
    turn = 1 - 2 * c
    ahead = dev(zz=(z + Z + turn) % Z)
    behind = dev(zz=(z + Z - turn) % Z)

    def slab(yy, zz):
        row = (yy % 2) * Z + zz
        col = pl.multiple_of((yy // 2) * 256, 256)
        return W1.at[row, c, :, pl.ds(col, 256)], W2.at[yy // 2, row, c]

    for i in range(1, 4):
        for w, (src, dst) in enumerate(zip((w1_in, w2_in), slab(y, z))):
            push(src, dst, ags.at[w, i], agr.at[w, mine], dev(yy=(y + i) % 4))

    def arrive(yy, zz):
        for w, ref in enumerate(slab(yy, zz)):
            wait(ref, agr.at[w, yy * Z + zz])

    def forward(yy, zz, k, to):
        for w, ref in enumerate(slab(yy, zz)):
            push(ref, ref, ags.at[w, k], agr.at[w, yy * Z + zz], to)

    def spread_first():
        for i in range(4):
            yy = (y + i) % 4
            if i:
                arrive(yy, z)
            forward(yy, z, 4 + i, ahead)
            forward(yy, z, 4 * half + 4 + i, behind)

    def spread(t):
        for i in range(4):
            yy = (y + i) % 4
            from_behind = (z + Z - turn * t) % Z
            from_ahead = (z + Z + turn * t) % Z
            arrive(yy, from_behind)
            forward(yy, from_behind, 4 + 4 * t + i, ahead)
            arrive(yy, from_ahead)

            @pl.when(t < half - 1)
            def _():
                forward(yy, from_ahead, 4 * half + 4 + 4 * t + i, behind)

    loop(0, CHUNKS, first)

    def relay(q, recv_kind, k, targets):
        for w, buf, _ in pair:
            got = part(buf, other, quarter[q], k)
            wait(got, wr.at[w, recv_kind, k])
            for kind, to in targets:
                push(got, got, ws.at[w, kind, k], wr.at[w, kind, k], to)

    def exchange(t):
        @pl.when(t < CHUNKS)
        def _():
            relay(0, 0, t, [(1, mate), (2, up), (3, partner)])

        @pl.when(jnp.logical_and(t >= 1, t < CHUNKS + 1))
        def _():
            relay(1, 1, t - 1, [(4, down), (5, partner)])

        @pl.when(jnp.logical_and(t >= 2, t < CHUNKS + 2))
        def _():
            relay(2, 2, t - 2, [(6, partner)])

        @pl.when(t >= 3)
        def _():
            relay(3, 4, t - 3, [(7, partner)])

    loop(0, CHUNKS + 3, exchange)

    local[4].wait()
    local[5].wait()
    spread_first()

    def partner_share(k):
        for q, kind in enumerate((3, 5, 6, 7)):
            for w, buf, _ in pair:
                theirs = part(buf, other, quarter[q] + (1 - 2 * c), k)
                wait(theirs, wr.at[w, kind, k])

    loop(0, CHUNKS, partner_share)
    wait(gains.at[other], gsem.at[1])
    for copy in local[:4] + local[6:]:
        copy.wait()

    def encode(m):
        @pl.when(x > 0)
        def _():
            wait(inbox.at[m], pir.at[m])

        @pl.when(x == 0)
        def _():
            inbox[m] = x0[m]

        def layer(j):
            h = inbox[m].astype(F32)
            scale = lax.rsqrt(jnp.mean(h * h, axis=-1, keepdims=True) + EPS)
            n = (h * scale * gains[j]).astype(BF16)
            u = jnp.dot(n, WI[j], preferred_element_type=F32)
            u = gelu(u).astype(BF16)
            r = (h + jnp.dot(u, WO[j], preferred_element_type=F32)).astype(BF16)

            @pl.when(j == 0)
            def _():
                inbox[m] = r

            @pl.when(j == 1)
            def _():
                outbox[m] = r

        loop(0, 2, layer)

        @pl.when(x < X - 1)
        def _():
            push(outbox.at[m], inbox.at[m], pis.at[m], pir.at[m], dev(xx=x + 1))

        @pl.when(jnp.logical_and(x == X - 1, m < X - 1))
        def _():
            push(outbox.at[m], feat, fs.at[m], fr, dev(xx=m))

        @pl.when(jnp.logical_and(x < X - 1, m < half - 1))
        def _():
            spread(m + 1)

    def project():
        @pl.when(x == X - 1)
        def _():
            loop(1, half, spread)

        for i in range(4):
            arrive((y + i) % 4, (z + half) % Z)
        push(W1.at[:, c], W1.at[:, c], pxs.at[0], pxr.at[0], partner)
        for h in range(2):
            push(W2.at[h, :, c], W2.at[h, :, c], pxs.at[1 + h], pxr.at[1 + h], partner)
        for i in range(1, X):
            xx = (x + i) % X
            wait(hid.at[xx], hr.at[xx])
        wait(W1.at[:, 1 - c], pxr.at[0])
        for h in range(2):
            wait(W2.at[h, :, 1 - c], pxr.at[1 + h])

        def block(j):
            w1 = W1[...].reshape(W1.shape[0] * 2 * W1.shape[2], W1.shape[3])
            w2 = W2[...].reshape(W2.shape[0] * W2.shape[1] * 2 * W2.shape[3], W2.shape[4])
            v = jnp.dot(hid[j], w1, preferred_element_type=F32)
            pre[j] = v
            a = (v / (1.0 + jnp.exp(-v))).astype(BF16)
            act[j] = a
            p = jnp.dot(a, w2, preferred_element_type=F32)

            @pl.when(j == x)
            def _():
                pown[...] = p

            @pl.when(j != x)
            def _():
                pbuf[j] = p.astype(BF16)
                push(pbuf.at[j], precv.at[x], pps.at[j], ppr.at[x], dev(xx=j))

        loop(0, X, block)

    def order(phase):
        @pl.when((phase == 0) == (x == X - 1))
        def _():
            project()

        @pl.when(phase == 0)
        def _():
            loop(0, X, encode)

    loop(0, 2, order)

    total = pown[...]
    for i in range(1, X):
        xx = (x + i) % X
        wait(precv.at[xx], ppr.at[xx])
        total = total + precv[xx].astype(F32)

    @pl.when(x < X - 1)
    def _():
        wait(feat, fr)

    @pl.when(x == X - 1)
    def _():
        feat[...] = outbox[X - 1]

    f = feat[...].astype(F32)
    squared = jnp.sum(total * total, axis=-1, keepdims=True) + EPS
    inv = lax.rsqrt(squared)
    unit = f * lax.rsqrt(jnp.sum(f * f, axis=-1, keepdims=True) + EPS)
    cosine = jnp.sum(total * unit, axis=-1, keepdims=True) * inv
    gall[x] = (cosine * total / squared - unit * inv).astype(BF16)
    for i in range(1, X):
        push(gall.at[x], gall.at[x], ggs.at[i], ggr.at[x], dev(xx=(x + i) % X))

    def back(i):
        j = (x + i) % X

        @pl.when(i > 0)
        def _():
            wait(gall.at[j], ggr.at[j])

        w2 = W2[...].reshape(W2.shape[0] * W2.shape[1] * 2 * W2.shape[3], W2.shape[4])
        b = lax.dot_general(gall[j], w2, (((1,), (1,)), ((), ())), preferred_element_type=F32)
        v = pre[j]
        s = 1.0 / (1.0 + jnp.exp(-v))
        gp[j] = (b * (s * (1.0 + v * (1.0 - s)))).astype(BF16)

    loop(0, X, back)

    tokens = X * T
    rows_dims = (((0,), (0,)), ((), ()))
    g2 = lax.dot_general(
        act[...].reshape(tokens, act.shape[2]),
        gall[...].reshape(tokens, D),
        rows_dims,
        preferred_element_type=F32,
    ).reshape(2, 2, Z, 2, 8, D)
    gpv = gp[...].reshape(tokens, gp.shape[2])
    span = Z // 2 * 2 * 64
    for q in range(4):
        g1 = lax.dot_general(
            hid[:, :, q * span : (q + 1) * span].reshape(tokens, span),
            gpv,
            rows_dims,
            preferred_element_type=F32,
        ).reshape(Z // 2, 2, 64, 512)
        yl2, z2 = q // 2, (q % 2) * (Z // 2)
        for cc in range(2):
            for yh2 in range(2):
                PB[cc, yh2 * 2 + yl2, z2 : z2 + Z // 2, 0:64, :] = g1[
                    :, cc, :, yh2 * 256 : yh2 * 256 + 256
                ].astype(BF16)
    for cc in range(2):
        for yy in range(4):
            for zz in range(Z):
                blk = g2[yy // 2, yy % 2, zz, cc]
                PB[cc, yy, zz, 64:96, :] = jnp.concatenate(
                    [blk[:, k * 256 : k * 256 + 256] for k in range(4)], axis=0
                ).astype(BF16)

    for yy in range(4):
        push(PB.at[1 - c, yy], crecv.at[yy], ccs.at[yy], ccr.at[yy], partner)

    def cores(yy):
        wait(crecv.at[yy], ccr.at[yy])
        S[yy] = (PB[c, yy].astype(F32) + crecv[yy].astype(F32)).astype(BF16)
        push(S.at[yy, (z + half) % Z], urecv.at[0, yy], us.at[0, yy], ur.at[0, yy], ahead)
        push(
            S.at[yy, (z + Z + turn * (half + 1)) % Z],
            drecv.at[0, yy],
            ds_.at[0, yy],
            dr.at[0, yy],
            behind,
        )

    loop(0, 4, cores)

    def ring(t):
        for yy in range(4):
            wait(urecv.at[t, yy], ur.at[t, yy])
            usend[t, yy] = (
                urecv[t, yy].astype(F32) + S[yy, (z + Z + turn * (half - 1 - t)) % Z].astype(F32)
            ).astype(BF16)
            push(usend.at[t, yy], urecv.at[t + 1, yy], us.at[t + 1, yy], ur.at[t + 1, yy], ahead)

            @pl.when(t < half - 2)
            def _():
                wait(drecv.at[t, yy], dr.at[t, yy])
                dsend[t, yy] = (
                    drecv[t, yy].astype(F32) + S[yy, (z + Z + turn * (half + 2 + t)) % Z].astype(F32)
                ).astype(BF16)
                push(
                    dsend.at[t, yy], drecv.at[t + 1, yy], ds_.at[t + 1, yy], dr.at[t + 1, yy], behind
                )

    loop(0, half - 1, ring)

    def rows(yy):
        wait(urecv.at[half - 1, yy], ur.at[half - 1, yy])
        wait(drecv.at[half - 2, yy], dr.at[half - 2, yy])
        r = (
            S[yy, z].astype(F32)
            + urecv[half - 1, yy].astype(F32)
            + drecv[half - 2, yy].astype(F32)
        )

        @pl.when(yy == y)
        def _():
            rown[...] = r

        @pl.when(yy != y)
        def _():
            rsend[yy] = r.astype(BF16)
            push(rsend.at[yy], yrecv.at[y], ys.at[yy], yr.at[y], dev(yy=yy))

    loop(0, 4, rows)
    r = rown[...]
    for i in range(1, 4):
        yy = (y + i) % 4
        wait(yrecv.at[yy], yr.at[yy])
        r = r + yrecv[yy].astype(F32)
    g1_out[...] = r[0:64]
    for k in range(4):
        g2_out[:, k * 256 : k * 256 + 256] = r[64 + 8 * k : 72 + 8 * k]

    for i in range(1, X):
        wait(hid.at[x], hs.at[i])
        wait(gall.at[x], ggs.at[i])
    wait(gains.at[yh], gsem.at[0])

    def sent_weights(k):
        for w, buf, _ in pair:
            for kind in range(8):
                wait(part(buf, 0, 0, k), ws.at[w, kind, k])

    loop(0, CHUNKS, sent_weights)

    def sent_gather(k):
        wait(w1_in, ags.at[0, k])
        wait(w2_in, ags.at[1, k])

    loop(1, 4 * Z, sent_gather)
    wait(W1.at[:, c], pxs.at[0])
    for h in range(2):
        wait(W2.at[h, :, c], pxs.at[1 + h])

    def sent_lines(m):
        @pl.when(x < X - 1)
        def _():
            wait(outbox.at[m], pis.at[m])

        @pl.when(jnp.logical_and(x == X - 1, m < X - 1))
        def _():
            wait(outbox.at[m], fs.at[m])

        @pl.when(m != x)
        def _():
            wait(pbuf.at[m], pps.at[m])

    loop(0, X, sent_lines)

    def sent_sums(yy):
        wait(crecv.at[yy], ccs.at[yy])
        for t in range(half):
            wait(urecv.at[0, yy], us.at[t, yy])
        for t in range(half - 1):
            wait(drecv.at[0, yy], ds_.at[t, yy])

        @pl.when(yy != y)
        def _():
            wait(rsend.at[yy], ys.at[yy])

    loop(0, 4, sent_sums)


def solution(mesh):
    X = mesh.shape["segment"] // 2
    Z = mesh.shape["dp"] // 4

    def on_device(x0, gain, wi, wo, hid, w1, w2):
        x0, wi, wo, hid = x0[0], wi[0], wo[0], hid[0]
        T, W = hid.shape
        N, D = x0.shape
        E = wi.shape[1]
        H = 2 * w1.shape[1]
        half = Z // 2
        B = (96, 256)
        vm = lambda shape, dtype=BF16: pltpu.VMEM(shape, dtype)
        dma = lambda *shape: pltpu.SemaphoreType.DMA(shape)
        scratch = [
            vm((2, D, E)),
            vm((2, E, D)),
            vm((2, 1, D), F32),
            vm((X, T, D)),
            vm((X, T, D)),
            vm((X, T, D)),
            vm((T, D)),
            vm((X, T, W)),
            vm((2 * Z, 2, 64, H)),
            vm((2, 2 * Z, 2, 8, D)),
            vm((X, T, H), F32),
            vm((X, T, H)),
            vm((X, T, D)),
            vm((T, D), F32),
            vm((X, T, D)),
            vm((X, T, D)),
            vm((X, T, H)),
            vm((2, 4, Z) + B),
            vm((4, Z) + B),
            vm((4, Z) + B),
            vm((half, 4) + B),
            vm((half - 1, 4) + B),
            vm((half - 1, 4) + B),
            vm((half - 2, 4) + B),
            vm((4,) + B),
            vm(B, F32),
            vm((4,) + B),
            dma(6 + X),
            dma(2),
            dma(2, 8, CHUNKS),
            dma(2, 8, CHUNKS),
            dma(X),
            dma(X),
            dma(2, 4 * Z),
            dma(2, 4 * Z),
            dma(3),
            dma(3),
            dma(X),
            dma(X),
            dma(X),
            pltpu.SemaphoreType.DMA,
            dma(X),
            dma(X),
            dma(X),
            dma(X),
            dma(4),
            dma(4),
            dma(half, 4),
            dma(half, 4),
            dma(half - 1, 4),
            dma(half - 1, 4),
            dma(4),
            dma(4),
        ]
        any_ = pl.BlockSpec(memory_space=pl.ANY)
        vmem = pl.BlockSpec(memory_space=pltpu.VMEM)
        return pl.pallas_call(
            functools.partial(mega, X, Z),
            out_shape=(
                jax.ShapeDtypeStruct((64, 256), F32),
                jax.ShapeDtypeStruct((8, D), F32),
            ),
            in_specs=[any_, vmem, any_, any_, any_, vmem, vmem],
            out_specs=(vmem, vmem),
            scratch_shapes=scratch,
            compiler_params=pltpu.CompilerParams(
                collective_id=0, has_side_effects=True, vmem_limit_bytes=62 << 20
            ),
        )(x0, gain, wi, wo, hid, w1, w2)

    placed = (
        P("dp", None, None),
        P("segment", None),
        P("segment", None, None),
        P("segment", None, None),
        P("dp", "segment", None),
        P("dp", "segment"),
        P(("segment", "dp"), None),
    )
    return jax.shard_map(
        on_device,
        mesh=mesh,
        in_specs=placed,
        out_specs=(P("dp", "segment"), P(("segment", "dp"), None)),
        check_vma=False,
    )
```

```python
import functools

import jax
import jax.numpy as jnp
from jax import lax
from jax.experimental import pallas as pl
from jax.experimental.pallas import tpu as pltpu
from jax.sharding import PartitionSpec as P

EPS = 1e-06
GELU_C = 0.7978845608
F32 = jnp.float32
BF16 = jnp.bfloat16
CHUNKS = 8


def gelu(v):
    return 0.5 * v * (1.0 + jnp.tanh(GELU_C * (v + 0.044715 * (v * v * v))))


def mega(
    X,
    Z,
    x0_in,
    gain_in,
    wi_in,
    wo_in,
    hid_in,
    w1_in,
    w2_in,
    g1_out,
    g2_out,
    WI,
    WO,
    gains,
    x0,
    inbox,
    outbox,
    feat,
    hid,
    W1,
    W2,
    pre,
    act,
    pbuf,
    pown,
    precv,
    gall,
    gp,
    PB,
    crecv,
    S,
    urecv,
    usend,
    drecv,
    dsend,
    rsend,
    rown,
    yrecv,
    lsem,
    gsem,
    ws,
    wr,
    hs,
    hr,
    ags,
    agr,
    pxs,
    pxr,
    pis,
    pir,
    fs,
    fr,
    pps,
    ppr,
    ggs,
    ggr,
    ccs,
    ccr,
    us,
    ur,
    ds_,
    dr,
    ys,
    yr,
):
    seg = lax.axis_index("segment")
    dp = lax.axis_index("dp")
    x = seg // 2
    yh = seg % 2
    yl = dp // (2 * Z)
    z = (dp // 2) % Z
    c = dp % 2
    y = yh * 2 + yl
    zp = z % 2
    T, D = hid.shape[1], x0.shape[2]

    def dev(xx=x, yy=y, zz=z, cc=c):
        return {
            "segment": xx * 2 + yy // 2,
            "dp": (yy % 2) * (2 * Z) + zz * 2 + cc,
        }

    def push(src, dst, ssem, rsem, to):
        pltpu.make_async_remote_copy(
            src_ref=src,
            dst_ref=dst,
            send_sem=ssem,
            recv_sem=rsem,
            device_id=to,
            device_id_type=pl.DeviceIdType.MESH,
        ).start()

    def wait(ref, sem):
        pltpu.make_async_copy(ref, ref, sem).wait()

    def loop(lo, hi, body):
        def step(i, carry):
            body(i)
            return carry

        lax.fori_loop(lo, hi, step, 0)

    partner = dev(cc=1 - c)
    cut = dev(yy=3 - y)
    mate = dev(yy=yh * 2 + (1 - yl))
    up = dev(zz=(z + 1) % Z)
    down = dev(zz=(z + Z - 1) % Z)

    local = [
        pltpu.make_async_copy(wi_in, WI.at[yh], lsem.at[0]),
        pltpu.make_async_copy(wo_in, WO.at[yh], lsem.at[1]),
        pltpu.make_async_copy(hid_in, hid.at[x], lsem.at[2]),
        pltpu.make_async_copy(gain_in, gains.at[yh], lsem.at[3]),
        pltpu.make_async_copy(
            w1_in, W1.at[yl * Z + z, c, :, pl.ds(pl.multiple_of(yh * 256, 256), 256)], lsem.at[4]
        ),
        pltpu.make_async_copy(w2_in, W2.at[yh, yl * Z + z, c], lsem.at[5]),
    ] + [
        pltpu.make_async_copy(
            x0_in.at[pl.ds(pl.multiple_of((2 * m + yh) * T, T), T), :], x0.at[m], lsem.at[6 + m]
        )
        for m in range(X)
    ]
    for copy in local:
        copy.start()

    barrier = pltpu.get_barrier_semaphore()

    def greet(to):
        pl.semaphore_signal(barrier, inc=1, device_id=to, device_id_type=pl.DeviceIdType.MESH)

    greet(partner)
    for i in range(1, X):
        greet(dev(xx=(x + i) % X))
    for i in range(1, 4):
        greet(dev(yy=(y + i) % 4))
    greet(up)
    greet(down)
    pl.semaphore_wait(barrier, 1 + (X - 1) + 3 + 2)

    for i in range(1, X):
        push(hid_in, hid.at[x], hs.at[i], hr.at[x], dev(xx=(x + i) % X))

    push(gain_in, gains.at[yh], gsem.at[0], gsem.at[1], cut)
    other = 1 - yh

    def part(ref, slot, piece, k):
        rows = ref.shape[1] // 8
        step = rows // CHUNKS
        if slot is None:
            return ref.at[pl.ds(pl.multiple_of(piece * rows + k * step, step), step), :]
        return ref.at[slot, pl.ds(pl.multiple_of(piece * rows + k * step, step), step), :]

    def native(ref, like, piece, k):
        rows = like.shape[1] // 8
        step = rows // CHUNKS
        return ref.at[pl.ds(pl.multiple_of(piece * rows + k * step, step), step), :]

    quarter_cut = 2 * (2 * zp + (1 - yl)) + c
    quarter = [
        2 * (2 * zp + yl) + c,
        2 * (2 * zp + (1 - yl)) + c,
        2 * (2 * (1 - zp) + yl) + c,
        2 * (2 * (1 - zp) + (1 - yl)) + c,
    ]
    pair = [(0, WI, wi_in), (1, WO, wo_in)]

    def first(k):
        for w, buf, src in pair:
            push(
                native(src, buf, quarter_cut, k),
                part(buf, yh, quarter_cut, k),
                ws.at[w, 0, k],
                wr.at[w, 0, k],
                cut,
            )

    mine = y * Z + z
    half = Z // 2
    turn = 1 - 2 * c
    ahead = dev(zz=(z + Z + turn) % Z)
    behind = dev(zz=(z + Z - turn) % Z)

    def slab(yy, zz):
        row = (yy % 2) * Z + zz
        col = pl.multiple_of((yy // 2) * 256, 256)
        return W1.at[row, c, :, pl.ds(col, 256)], W2.at[yy // 2, row, c]

    for i in range(1, 4):
        for w, (src, dst) in enumerate(zip((w1_in, w2_in), slab(y, z))):
            push(src, dst, ags.at[w, i], agr.at[w, mine], dev(yy=(y + i) % 4))

    def arrive(yy, zz):
        for w, ref in enumerate(slab(yy, zz)):
            wait(ref, agr.at[w, yy * Z + zz])

    def forward(yy, zz, k, to):
        for w, ref in enumerate(slab(yy, zz)):
            push(ref, ref, ags.at[w, k], agr.at[w, yy * Z + zz], to)

    def spread_first():
        for i in range(4):
            yy = (y + i) % 4
            if i:
                arrive(yy, z)
            forward(yy, z, 4 + i, ahead)
            forward(yy, z, 4 * half + 4 + i, behind)

    def spread(t):
        for i in range(4):
            yy = (y + i) % 4
            from_behind = (z + Z - turn * t) % Z
            from_ahead = (z + Z + turn * t) % Z
            arrive(yy, from_behind)
            forward(yy, from_behind, 4 + 4 * t + i, ahead)
            arrive(yy, from_ahead)

            @pl.when(t < half - 1)
            def _():
                forward(yy, from_ahead, 4 * half + 4 + 4 * t + i, behind)

    loop(0, CHUNKS, first)

    def relay(q, recv_kind, k, targets):
        for w, buf, _ in pair:
            got = part(buf, other, quarter[q], k)
            wait(got, wr.at[w, recv_kind, k])
            for kind, to in targets:
                push(got, got, ws.at[w, kind, k], wr.at[w, kind, k], to)

    def exchange(t):
        @pl.when(t < CHUNKS)
        def _():
            relay(0, 0, t, [(1, mate), (2, up), (3, partner)])

        @pl.when(jnp.logical_and(t >= 1, t < CHUNKS + 1))
        def _():
            relay(1, 1, t - 1, [(4, down), (5, partner)])

        @pl.when(jnp.logical_and(t >= 2, t < CHUNKS + 2))
        def _():
            relay(2, 2, t - 2, [(6, partner)])

        @pl.when(t >= 3)
        def _():
            relay(3, 4, t - 3, [(7, partner)])

    loop(0, CHUNKS + 3, exchange)

    local[4].wait()
    local[5].wait()
    spread_first()

    def partner_share(k):
        for q, kind in enumerate((3, 5, 6, 7)):
            for w, buf, _ in pair:
                theirs = part(buf, other, quarter[q] + (1 - 2 * c), k)
                wait(theirs, wr.at[w, kind, k])

    loop(0, CHUNKS, partner_share)
    wait(gains.at[other], gsem.at[1])
    for copy in local[:4] + local[6:]:
        copy.wait()

    def encode(m):
        @pl.when(x > 0)
        def _():
            wait(inbox.at[m], pir.at[m])

        @pl.when(x == 0)
        def _():
            inbox[m] = x0[m]

        def layer(j):
            h = inbox[m].astype(F32)
            scale = lax.rsqrt(jnp.mean(h * h, axis=-1, keepdims=True) + EPS)
            n = (h * scale * gains[j]).astype(BF16)
            u = jnp.dot(n, WI[j], preferred_element_type=F32)
            u = gelu(u).astype(BF16)
            r = (h + jnp.dot(u, WO[j], preferred_element_type=F32)).astype(BF16)

            @pl.when(j == 0)
            def _():
                inbox[m] = r

            @pl.when(j == 1)
            def _():
                outbox[m] = r

        loop(0, 2, layer)

        @pl.when(x < X - 1)
        def _():
            push(outbox.at[m], inbox.at[m], pis.at[m], pir.at[m], dev(xx=x + 1))

        @pl.when(jnp.logical_and(x == X - 1, m < X - 1))
        def _():
            push(outbox.at[m], feat, fs.at[m], fr, dev(xx=m))

        @pl.when(jnp.logical_and(x < X - 1, m < half - 1))
        def _():
            spread(m + 1)

    def project():
        @pl.when(x == X - 1)
        def _():
            loop(1, half, spread)

        for i in range(4):
            arrive((y + i) % 4, (z + half) % Z)
        push(W1.at[:, c], W1.at[:, c], pxs.at[0], pxr.at[0], partner)
        for h in range(2):
            push(W2.at[h, :, c], W2.at[h, :, c], pxs.at[1 + h], pxr.at[1 + h], partner)
        for i in range(1, X):
            xx = (x + i) % X
            wait(hid.at[xx], hr.at[xx])
        wait(W1.at[:, 1 - c], pxr.at[0])
        for h in range(2):
            wait(W2.at[h, :, 1 - c], pxr.at[1 + h])

        def block(j):
            w1 = W1[...].reshape(W1.shape[0] * 2 * W1.shape[2], W1.shape[3])
            w2 = W2[...].reshape(W2.shape[0] * W2.shape[1] * 2 * W2.shape[3], W2.shape[4])
            v = jnp.dot(hid[j], w1, preferred_element_type=F32)
            pre[j] = v
            a = (v / (1.0 + jnp.exp(-v))).astype(BF16)
            act[j] = a
            p = jnp.dot(a, w2, preferred_element_type=F32)

            @pl.when(j == x)
            def _():
                pown[...] = p

            @pl.when(j != x)
            def _():
                pbuf[j] = p.astype(BF16)
                push(pbuf.at[j], precv.at[x], pps.at[j], ppr.at[x], dev(xx=j))

        loop(0, X, block)

    def order(phase):
        @pl.when((phase == 0) == (x == X - 1))
        def _():
            project()

        @pl.when(phase == 0)
        def _():
            loop(0, X, encode)

    loop(0, 2, order)

    total = pown[...]
    for i in range(1, X):
        xx = (x + i) % X
        wait(precv.at[xx], ppr.at[xx])
        total = total + precv[xx].astype(F32)

    @pl.when(x < X - 1)
    def _():
        wait(feat, fr)

    @pl.when(x == X - 1)
    def _():
        feat[...] = outbox[X - 1]

    f = feat[...].astype(F32)
    squared = jnp.sum(total * total, axis=-1, keepdims=True) + EPS
    inv = lax.rsqrt(squared)
    unit = f * lax.rsqrt(jnp.sum(f * f, axis=-1, keepdims=True) + EPS)
    cosine = jnp.sum(total * unit, axis=-1, keepdims=True) * inv
    gall[x] = (cosine * total / squared - unit * inv).astype(BF16)
    for i in range(1, X):
        push(gall.at[x], gall.at[x], ggs.at[i], ggr.at[x], dev(xx=(x + i) % X))

    def back(i):
        j = (x + i) % X

        @pl.when(i > 0)
        def _():
            wait(gall.at[j], ggr.at[j])

        w2 = W2[...].reshape(W2.shape[0] * W2.shape[1] * 2 * W2.shape[3], W2.shape[4])
        b = lax.dot_general(gall[j], w2, (((1,), (1,)), ((), ())), preferred_element_type=F32)
        v = pre[j]
        s = 1.0 / (1.0 + jnp.exp(-v))
        gp[j] = (b * (s * (1.0 + v * (1.0 - s)))).astype(BF16)

    loop(0, X, back)

    tokens = X * T
    rows_dims = (((0,), (0,)), ((), ()))
    g2 = lax.dot_general(
        act[...].reshape(tokens, act.shape[2]),
        gall[...].reshape(tokens, D),
        rows_dims,
        preferred_element_type=F32,
    ).reshape(2, 2, Z, 2, 8, D)
    gpv = gp[...].reshape(tokens, gp.shape[2])
    for cc in range(2):
        for yy in range(4):
            for zz in range(Z):
                blk = g2[yy // 2, yy % 2, zz, cc]
                PB[cc, yy, zz, 64:96, :] = jnp.concatenate(
                    [blk[:, k * 256 : k * 256 + 256] for k in range(4)], axis=0
                ).astype(BF16)

    def swap(yy):
        push(PB.at[1 - c, yy], crecv.at[yy], ccs.at[yy], ccr.at[yy], partner)

    def cores(yy):
        wait(crecv.at[yy], ccr.at[yy])
        S[yy] = (PB[c, yy].astype(F32) + crecv[yy].astype(F32)).astype(BF16)
        push(S.at[yy, (z + half) % Z], urecv.at[0, yy], us.at[0, yy], ur.at[0, yy], ahead)
        push(
            S.at[yy, (z + Z + turn * (half + 1)) % Z],
            drecv.at[0, yy],
            ds_.at[0, yy],
            dr.at[0, yy],
            behind,
        )

    span = Z // 2 * 2 * 64
    for q in range(4):
        g1 = lax.dot_general(
            hid[:, :, q * span : (q + 1) * span].reshape(tokens, span),
            gpv,
            rows_dims,
            preferred_element_type=F32,
        ).reshape(Z // 2, 2, 64, 512)
        yl2, z2 = q // 2, (q % 2) * (Z // 2)
        for cc in range(2):
            for yh2 in range(2):
                PB[cc, yh2 * 2 + yl2, z2 : z2 + Z // 2, 0:64, :] = g1[
                    :, cc, :, yh2 * 256 : yh2 * 256 + 256
                ].astype(BF16)
        if q % 2:
            swap(yl2)
            swap(2 + yl2)
        if q == 2:
            loop(0, 2, lambda i: cores(2 * i))
    loop(0, 2, lambda i: cores(2 * i + 1))

    def ring(t):
        for yy in (0, 2, 1, 3):
            wait(urecv.at[t, yy], ur.at[t, yy])
            usend[t, yy] = (
                urecv[t, yy].astype(F32) + S[yy, (z + Z + turn * (half - 1 - t)) % Z].astype(F32)
            ).astype(BF16)
            push(usend.at[t, yy], urecv.at[t + 1, yy], us.at[t + 1, yy], ur.at[t + 1, yy], ahead)

            @pl.when(t < half - 2)
            def _():
                wait(drecv.at[t, yy], dr.at[t, yy])
                dsend[t, yy] = (
                    drecv[t, yy].astype(F32) + S[yy, (z + Z + turn * (half + 2 + t)) % Z].astype(F32)
                ).astype(BF16)
                push(
                    dsend.at[t, yy], drecv.at[t + 1, yy], ds_.at[t + 1, yy], dr.at[t + 1, yy], behind
                )

    loop(0, half - 1, ring)

    def rows(yy):
        wait(urecv.at[half - 1, yy], ur.at[half - 1, yy])
        wait(drecv.at[half - 2, yy], dr.at[half - 2, yy])
        r = (
            S[yy, z].astype(F32)
            + urecv[half - 1, yy].astype(F32)
            + drecv[half - 2, yy].astype(F32)
        )

        @pl.when(yy == y)
        def _():
            rown[...] = r

        @pl.when(yy != y)
        def _():
            rsend[yy] = r.astype(BF16)
            push(rsend.at[yy], yrecv.at[y], ys.at[yy], yr.at[y], dev(yy=yy))

    loop(0, 4, rows)
    r = rown[...]
    for i in range(1, 4):
        yy = (y + i) % 4
        wait(yrecv.at[yy], yr.at[yy])
        r = r + yrecv[yy].astype(F32)
    g1_out[...] = r[0:64]
    for k in range(4):
        g2_out[:, k * 256 : k * 256 + 256] = r[64 + 8 * k : 72 + 8 * k]

    for i in range(1, X):
        wait(hid.at[x], hs.at[i])
        wait(gall.at[x], ggs.at[i])
    wait(gains.at[yh], gsem.at[0])

    def sent_weights(k):
        for w, buf, _ in pair:
            for kind in range(8):
                wait(part(buf, 0, 0, k), ws.at[w, kind, k])

    loop(0, CHUNKS, sent_weights)

    def sent_gather(k):
        wait(w1_in, ags.at[0, k])
        wait(w2_in, ags.at[1, k])

    loop(1, 4 * Z, sent_gather)
    wait(W1.at[:, c], pxs.at[0])
    for h in range(2):
        wait(W2.at[h, :, c], pxs.at[1 + h])

    def sent_lines(m):
        @pl.when(x < X - 1)
        def _():
            wait(outbox.at[m], pis.at[m])

        @pl.when(jnp.logical_and(x == X - 1, m < X - 1))
        def _():
            wait(outbox.at[m], fs.at[m])

        @pl.when(m != x)
        def _():
            wait(pbuf.at[m], pps.at[m])

    loop(0, X, sent_lines)

    def sent_sums(yy):
        wait(crecv.at[yy], ccs.at[yy])
        for t in range(half):
            wait(urecv.at[0, yy], us.at[t, yy])
        for t in range(half - 1):
            wait(drecv.at[0, yy], ds_.at[t, yy])

        @pl.when(yy != y)
        def _():
            wait(rsend.at[yy], ys.at[yy])

    loop(0, 4, sent_sums)


def solution(mesh):
    X = mesh.shape["segment"] // 2
    Z = mesh.shape["dp"] // 4

    def on_device(x0, gain, wi, wo, hid, w1, w2):
        x0, wi, wo, hid = x0[0], wi[0], wo[0], hid[0]
        T, W = hid.shape
        N, D = x0.shape
        E = wi.shape[1]
        H = 2 * w1.shape[1]
        half = Z // 2
        B = (96, 256)
        vm = lambda shape, dtype=BF16: pltpu.VMEM(shape, dtype)
        dma = lambda *shape: pltpu.SemaphoreType.DMA(shape)
        scratch = [
            vm((2, D, E)),
            vm((2, E, D)),
            vm((2, 1, D), F32),
            vm((X, T, D)),
            vm((X, T, D)),
            vm((X, T, D)),
            vm((T, D)),
            vm((X, T, W)),
            vm((2 * Z, 2, 64, H)),
            vm((2, 2 * Z, 2, 8, D)),
            vm((X, T, H), F32),
            vm((X, T, H)),
            vm((X, T, D)),
            vm((T, D), F32),
            vm((X, T, D)),
            vm((X, T, D)),
            vm((X, T, H)),
            vm((2, 4, Z) + B),
            vm((4, Z) + B),
            vm((4, Z) + B),
            vm((half, 4) + B),
            vm((half - 1, 4) + B),
            vm((half - 1, 4) + B),
            vm((half - 2, 4) + B),
            vm((4,) + B),
            vm(B, F32),
            vm((4,) + B),
            dma(6 + X),
            dma(2),
            dma(2, 8, CHUNKS),
            dma(2, 8, CHUNKS),
            dma(X),
            dma(X),
            dma(2, 4 * Z),
            dma(2, 4 * Z),
            dma(3),
            dma(3),
            dma(X),
            dma(X),
            dma(X),
            pltpu.SemaphoreType.DMA,
            dma(X),
            dma(X),
            dma(X),
            dma(X),
            dma(4),
            dma(4),
            dma(half, 4),
            dma(half, 4),
            dma(half - 1, 4),
            dma(half - 1, 4),
            dma(4),
            dma(4),
        ]
        any_ = pl.BlockSpec(memory_space=pl.ANY)
        vmem = pl.BlockSpec(memory_space=pltpu.VMEM)
        return pl.pallas_call(
            functools.partial(mega, X, Z),
            out_shape=(
                jax.ShapeDtypeStruct((64, 256), F32),
                jax.ShapeDtypeStruct((8, D), F32),
            ),
            in_specs=[any_] * 7,
            out_specs=(vmem, vmem),
            scratch_shapes=scratch,
            compiler_params=pltpu.CompilerParams(
                collective_id=0, has_side_effects=True, vmem_limit_bytes=62 << 20
            ),
        )(x0, gain, wi, wo, hid, w1, w2)

    placed = (
        P("dp", None, None),
        P("segment", None),
        P("segment", None, None),
        P("segment", None, None),
        P("dp", "segment", None),
        P("dp", "segment"),
        P(("segment", "dp"), None),
    )
    return jax.shard_map(
        on_device,
        mesh=mesh,
        in_specs=placed,
        out_specs=(P("dp", "segment"), P(("segment", "dp"), None)),
        check_vma=False,
    )
```

```python
import functools

import jax
import jax.numpy as jnp
from jax import lax
from jax.experimental import pallas as pl
from jax.experimental.pallas import tpu as pltpu
from jax.sharding import PartitionSpec as P

EPS = 1e-06
GELU_C = 0.7978845608
F32 = jnp.float32
BF16 = jnp.bfloat16
CHUNKS = 4


def gelu(v):
    return 0.5 * v * (1.0 + jnp.tanh(GELU_C * (v + 0.044715 * (v * v * v))))


def mega(
    X,
    Z,
    x0_in,
    gain_in,
    wi_in,
    wo_in,
    hid_in,
    w1_in,
    w2_in,
    g1_out,
    g2_out,
    WI,
    WO,
    gains,
    x0,
    inbox,
    outbox,
    feat,
    hid,
    W1,
    W2,
    pre,
    act,
    pbuf,
    pown,
    precv,
    gall,
    gp,
    PB,
    crecv,
    S,
    urecv,
    usend,
    drecv,
    dsend,
    rsend,
    rown,
    yrecv,
    lsem,
    gsem,
    ws,
    wr,
    hs,
    hr,
    ags,
    agr,
    pxs,
    pxr,
    pis,
    pir,
    fs,
    fr,
    pps,
    ppr,
    ggs,
    ggr,
    ccs,
    ccr,
    us,
    ur,
    ds_,
    dr,
    ys,
    yr,
):
    seg = lax.axis_index("segment")
    dp = lax.axis_index("dp")
    x = seg // 2
    yh = seg % 2
    yl = dp // (2 * Z)
    z = (dp // 2) % Z
    c = dp % 2
    y = yh * 2 + yl
    zp = z % 2
    T, D = hid.shape[1], x0.shape[2]

    def dev(xx=x, yy=y, zz=z, cc=c):
        return {
            "segment": xx * 2 + yy // 2,
            "dp": (yy % 2) * (2 * Z) + zz * 2 + cc,
        }

    def push(src, dst, ssem, rsem, to):
        pltpu.make_async_remote_copy(
            src_ref=src,
            dst_ref=dst,
            send_sem=ssem,
            recv_sem=rsem,
            device_id=to,
            device_id_type=pl.DeviceIdType.MESH,
        ).start()

    def wait(ref, sem):
        pltpu.make_async_copy(ref, ref, sem).wait()

    def loop(lo, hi, body):
        def step(i, carry):
            body(i)
            return carry

        lax.fori_loop(lo, hi, step, 0)

    partner = dev(cc=1 - c)
    cut = dev(yy=3 - y)
    mate = dev(yy=yh * 2 + (1 - yl))
    up = dev(zz=(z + 1) % Z)
    down = dev(zz=(z + Z - 1) % Z)

    local = [
        pltpu.make_async_copy(wi_in, WI.at[yh], lsem.at[0]),
        pltpu.make_async_copy(wo_in, WO.at[yh], lsem.at[1]),
        pltpu.make_async_copy(hid_in, hid.at[x], lsem.at[2]),
        pltpu.make_async_copy(gain_in, gains.at[yh], lsem.at[3]),
        pltpu.make_async_copy(
            w1_in, W1.at[yl * Z + z, c, :, pl.ds(pl.multiple_of(yh * 256, 256), 256)], lsem.at[4]
        ),
        pltpu.make_async_copy(w2_in, W2.at[yh, yl * Z + z, c], lsem.at[5]),
    ] + [
        pltpu.make_async_copy(
            x0_in.at[pl.ds(pl.multiple_of((2 * m + yh) * T, T), T), :], x0.at[m], lsem.at[6 + m]
        )
        for m in range(X)
    ]
    for copy in local:
        copy.start()

    barrier = pltpu.get_barrier_semaphore()

    def greet(to):
        pl.semaphore_signal(barrier, inc=1, device_id=to, device_id_type=pl.DeviceIdType.MESH)

    greet(partner)
    for i in range(1, X):
        greet(dev(xx=(x + i) % X))
    for i in range(1, 4):
        greet(dev(yy=(y + i) % 4))
    greet(up)
    greet(down)
    pl.semaphore_wait(barrier, 1 + (X - 1) + 3 + 2)

    for i in range(1, X):
        push(hid_in, hid.at[x], hs.at[i], hr.at[x], dev(xx=(x + i) % X))

    push(gain_in, gains.at[yh], gsem.at[0], gsem.at[1], cut)
    other = 1 - yh

    def part(ref, slot, piece, k):
        rows = ref.shape[1] // 8
        step = rows // CHUNKS
        if slot is None:
            return ref.at[pl.ds(pl.multiple_of(piece * rows + k * step, step), step), :]
        return ref.at[slot, pl.ds(pl.multiple_of(piece * rows + k * step, step), step), :]

    def native(ref, like, piece, k):
        rows = like.shape[1] // 8
        step = rows // CHUNKS
        return ref.at[pl.ds(pl.multiple_of(piece * rows + k * step, step), step), :]

    quarter_cut = 2 * (2 * zp + (1 - yl)) + c
    quarter = [
        2 * (2 * zp + yl) + c,
        2 * (2 * zp + (1 - yl)) + c,
        2 * (2 * (1 - zp) + yl) + c,
        2 * (2 * (1 - zp) + (1 - yl)) + c,
    ]
    pair = [(0, WI, wi_in), (1, WO, wo_in)]

    def first(k):
        for w, buf, src in pair:
            push(
                native(src, buf, quarter_cut, k),
                part(buf, yh, quarter_cut, k),
                ws.at[w, 0, k],
                wr.at[w, 0, k],
                cut,
            )

    mine = y * Z + z
    half = Z // 2
    turn = 1 - 2 * c
    ahead = dev(zz=(z + Z + turn) % Z)
    behind = dev(zz=(z + Z - turn) % Z)

    def slab(yy, zz):
        row = (yy % 2) * Z + zz
        col = pl.multiple_of((yy // 2) * 256, 256)
        return W1.at[row, c, :, pl.ds(col, 256)], W2.at[yy // 2, row, c]

    for i in range(1, 4):
        for w, (src, dst) in enumerate(zip((w1_in, w2_in), slab(y, z))):
            push(src, dst, ags.at[w, i], agr.at[w, mine], dev(yy=(y + i) % 4))

    def arrive(yy, zz):
        for w, ref in enumerate(slab(yy, zz)):
            wait(ref, agr.at[w, yy * Z + zz])

    def forward(yy, zz, k, to):
        for w, ref in enumerate(slab(yy, zz)):
            push(ref, ref, ags.at[w, k], agr.at[w, yy * Z + zz], to)

    def spread_first():
        for i in range(4):
            yy = (y + i) % 4
            if i:
                arrive(yy, z)
            forward(yy, z, 4 + i, ahead)
            forward(yy, z, 4 * half + 4 + i, behind)

    def spread(t):
        for i in range(4):
            yy = (y + i) % 4
            from_behind = (z + Z - turn * t) % Z
            from_ahead = (z + Z + turn * t) % Z
            arrive(yy, from_behind)
            forward(yy, from_behind, 4 + 4 * t + i, ahead)
            arrive(yy, from_ahead)

            @pl.when(t < half - 1)
            def _():
                forward(yy, from_ahead, 4 * half + 4 + 4 * t + i, behind)

    loop(0, CHUNKS, first)

    def relay(q, recv_kind, k, targets):
        for w, buf, _ in pair:
            got = part(buf, other, quarter[q], k)
            wait(got, wr.at[w, recv_kind, k])
            for kind, to in targets:
                push(got, got, ws.at[w, kind, k], wr.at[w, kind, k], to)

    def exchange(t):
        @pl.when(t < CHUNKS)
        def _():
            relay(0, 0, t, [(1, mate), (2, up), (3, partner)])

        @pl.when(jnp.logical_and(t >= 1, t < CHUNKS + 1))
        def _():
            relay(1, 1, t - 1, [(4, down), (5, partner)])

        @pl.when(jnp.logical_and(t >= 2, t < CHUNKS + 2))
        def _():
            relay(2, 2, t - 2, [(6, partner)])

        @pl.when(t >= 3)
        def _():
            relay(3, 4, t - 3, [(7, partner)])

    loop(0, CHUNKS + 3, exchange)

    local[4].wait()
    local[5].wait()
    spread_first()

    def partner_share(k):
        for q, kind in enumerate((3, 5, 6, 7)):
            for w, buf, _ in pair:
                theirs = part(buf, other, quarter[q] + (1 - 2 * c), k)
                wait(theirs, wr.at[w, kind, k])

    loop(0, CHUNKS, partner_share)
    wait(gains.at[other], gsem.at[1])
    for copy in local[:4] + local[6:]:
        copy.wait()

    def encode(m):
        @pl.when(x > 0)
        def _():
            wait(inbox.at[m], pir.at[m])

        @pl.when(x == 0)
        def _():
            inbox[m] = x0[m]

        def layer(j):
            h = inbox[m].astype(F32)
            scale = lax.rsqrt(jnp.mean(h * h, axis=-1, keepdims=True) + EPS)
            n = (h * scale * gains[j]).astype(BF16)
            u = jnp.dot(n, WI[j], preferred_element_type=F32)
            u = gelu(u).astype(BF16)
            r = (h + jnp.dot(u, WO[j], preferred_element_type=F32)).astype(BF16)

            @pl.when(j == 0)
            def _():
                inbox[m] = r

            @pl.when(j == 1)
            def _():
                outbox[m] = r

        loop(0, 2, layer)

        @pl.when(x < X - 1)
        def _():
            push(outbox.at[m], inbox.at[m], pis.at[m], pir.at[m], dev(xx=x + 1))

        @pl.when(jnp.logical_and(x == X - 1, m < X - 1))
        def _():
            push(outbox.at[m], feat, fs.at[m], fr, dev(xx=m))

        @pl.when(jnp.logical_and(x < X - 1, m < half - 1))
        def _():
            spread(m + 1)

    def project():
        @pl.when(x == X - 1)
        def _():
            loop(1, half, spread)

        for i in range(4):
            arrive((y + i) % 4, (z + half) % Z)
        push(W1.at[:, c], W1.at[:, c], pxs.at[0], pxr.at[0], partner)
        for h in range(2):
            push(W2.at[h, :, c], W2.at[h, :, c], pxs.at[1 + h], pxr.at[1 + h], partner)
        for i in range(1, X):
            xx = (x + i) % X
            wait(hid.at[xx], hr.at[xx])
        wait(W1.at[:, 1 - c], pxr.at[0])
        for h in range(2):
            wait(W2.at[h, :, 1 - c], pxr.at[1 + h])

        def block(j):
            w1 = W1[...].reshape(W1.shape[0] * 2 * W1.shape[2], W1.shape[3])
            w2 = W2[...].reshape(W2.shape[0] * W2.shape[1] * 2 * W2.shape[3], W2.shape[4])
            v = jnp.dot(hid[j], w1, preferred_element_type=F32)
            pre[j] = v
            a = (v / (1.0 + jnp.exp(-v))).astype(BF16)
            act[j] = a
            p = jnp.dot(a, w2, preferred_element_type=F32)

            @pl.when(j == x)
            def _():
                pown[...] = p

            @pl.when(j != x)
            def _():
                pbuf[j] = p.astype(BF16)
                push(pbuf.at[j], precv.at[x], pps.at[j], ppr.at[x], dev(xx=j))

        loop(0, X, block)

    def order(phase):
        @pl.when((phase == 0) == (x == X - 1))
        def _():
            project()

        @pl.when(phase == 0)
        def _():
            loop(0, X, encode)

    loop(0, 2, order)

    total = pown[...]
    for i in range(1, X):
        xx = (x + i) % X
        wait(precv.at[xx], ppr.at[xx])
        total = total + precv[xx].astype(F32)

    @pl.when(x < X - 1)
    def _():
        wait(feat, fr)

    @pl.when(x == X - 1)
    def _():
        feat[...] = outbox[X - 1]

    f = feat[...].astype(F32)
    squared = jnp.sum(total * total, axis=-1, keepdims=True) + EPS
    inv = lax.rsqrt(squared)
    unit = f * lax.rsqrt(jnp.sum(f * f, axis=-1, keepdims=True) + EPS)
    cosine = jnp.sum(total * unit, axis=-1, keepdims=True) * inv
    gall[x] = (cosine * total / squared - unit * inv).astype(BF16)
    for i in range(1, X):
        push(gall.at[x], gall.at[x], ggs.at[i], ggr.at[x], dev(xx=(x + i) % X))

    def back(i):
        j = (x + i) % X

        @pl.when(i > 0)
        def _():
            wait(gall.at[j], ggr.at[j])

        w2 = W2[...].reshape(W2.shape[0] * W2.shape[1] * 2 * W2.shape[3], W2.shape[4])
        b = lax.dot_general(gall[j], w2, (((1,), (1,)), ((), ())), preferred_element_type=F32)
        v = pre[j]
        s = 1.0 / (1.0 + jnp.exp(-v))
        gp[j] = (b * (s * (1.0 + v * (1.0 - s)))).astype(BF16)

    loop(0, X, back)

    tokens = X * T
    rows_dims = (((0,), (0,)), ((), ()))
    g2 = lax.dot_general(
        act[...].reshape(tokens, act.shape[2]),
        gall[...].reshape(tokens, D),
        rows_dims,
        preferred_element_type=F32,
    ).reshape(2, 2, Z, 2, 8, D)
    gpv = gp[...].reshape(tokens, gp.shape[2])
    for cc in range(2):
        for yy in range(4):
            for zz in range(Z):
                blk = g2[yy // 2, yy % 2, zz, cc]
                PB[cc, yy, zz, 64:96, :] = jnp.concatenate(
                    [blk[:, k * 256 : k * 256 + 256] for k in range(4)], axis=0
                ).astype(BF16)

    def swap(yy):
        push(PB.at[1 - c, yy], crecv.at[yy], ccs.at[yy], ccr.at[yy], partner)

    def cores(yy):
        wait(crecv.at[yy], ccr.at[yy])
        S[yy] = (PB[c, yy].astype(F32) + crecv[yy].astype(F32)).astype(BF16)
        push(S.at[yy, (z + half) % Z], urecv.at[0, yy], us.at[0, yy], ur.at[0, yy], ahead)
        push(
            S.at[yy, (z + Z + turn * (half + 1)) % Z],
            drecv.at[0, yy],
            ds_.at[0, yy],
            dr.at[0, yy],
            behind,
        )

    span = Z // 2 * 2 * 64
    for q in range(4):
        g1 = lax.dot_general(
            hid[:, :, q * span : (q + 1) * span].reshape(tokens, span),
            gpv,
            rows_dims,
            preferred_element_type=F32,
        ).reshape(Z // 2, 2, 64, 512)
        yl2, z2 = q // 2, (q % 2) * (Z // 2)
        for cc in range(2):
            for yh2 in range(2):
                PB[cc, yh2 * 2 + yl2, z2 : z2 + Z // 2, 0:64, :] = g1[
                    :, cc, :, yh2 * 256 : yh2 * 256 + 256
                ].astype(BF16)
        if q % 2:
            swap(yl2)
            swap(2 + yl2)
        if q == 2:
            loop(0, 2, lambda i: cores(2 * i))
    loop(0, 2, lambda i: cores(2 * i + 1))

    def ring(t):
        for yy in (0, 2, 1, 3):
            wait(urecv.at[t, yy], ur.at[t, yy])
            usend[t, yy] = (
                urecv[t, yy].astype(F32) + S[yy, (z + Z + turn * (half - 1 - t)) % Z].astype(F32)
            ).astype(BF16)
            push(usend.at[t, yy], urecv.at[t + 1, yy], us.at[t + 1, yy], ur.at[t + 1, yy], ahead)

            @pl.when(t < half - 2)
            def _():
                wait(drecv.at[t, yy], dr.at[t, yy])
                dsend[t, yy] = (
                    drecv[t, yy].astype(F32) + S[yy, (z + Z + turn * (half + 2 + t)) % Z].astype(F32)
                ).astype(BF16)
                push(
                    dsend.at[t, yy], drecv.at[t + 1, yy], ds_.at[t + 1, yy], dr.at[t + 1, yy], behind
                )

    loop(0, half - 1, ring)

    def rows(yy):
        wait(urecv.at[half - 1, yy], ur.at[half - 1, yy])
        wait(drecv.at[half - 2, yy], dr.at[half - 2, yy])
        r = (
            S[yy, z].astype(F32)
            + urecv[half - 1, yy].astype(F32)
            + drecv[half - 2, yy].astype(F32)
        )

        @pl.when(yy == y)
        def _():
            rown[...] = r

        @pl.when(yy != y)
        def _():
            rsend[yy] = r.astype(BF16)
            push(rsend.at[yy], yrecv.at[y], ys.at[yy], yr.at[y], dev(yy=yy))

    loop(0, 4, rows)
    r = rown[...]
    for i in range(1, 4):
        yy = (y + i) % 4
        wait(yrecv.at[yy], yr.at[yy])
        r = r + yrecv[yy].astype(F32)
    g1_out[...] = r[0:64]
    for k in range(4):
        g2_out[:, k * 256 : k * 256 + 256] = r[64 + 8 * k : 72 + 8 * k]

    for i in range(1, X):
        wait(hid.at[x], hs.at[i])
        wait(gall.at[x], ggs.at[i])
    wait(gains.at[yh], gsem.at[0])

    def sent_weights(k):
        for w, buf, _ in pair:
            for kind in range(8):
                wait(part(buf, 0, 0, k), ws.at[w, kind, k])

    loop(0, CHUNKS, sent_weights)

    def sent_gather(k):
        wait(w1_in, ags.at[0, k])
        wait(w2_in, ags.at[1, k])

    loop(1, 4 * Z, sent_gather)
    wait(W1.at[:, c], pxs.at[0])
    for h in range(2):
        wait(W2.at[h, :, c], pxs.at[1 + h])

    def sent_lines(m):
        @pl.when(x < X - 1)
        def _():
            wait(outbox.at[m], pis.at[m])

        @pl.when(jnp.logical_and(x == X - 1, m < X - 1))
        def _():
            wait(outbox.at[m], fs.at[m])

        @pl.when(m != x)
        def _():
            wait(pbuf.at[m], pps.at[m])

    loop(0, X, sent_lines)

    def sent_sums(yy):
        wait(crecv.at[yy], ccs.at[yy])
        for t in range(half):
            wait(urecv.at[0, yy], us.at[t, yy])
        for t in range(half - 1):
            wait(drecv.at[0, yy], ds_.at[t, yy])

        @pl.when(yy != y)
        def _():
            wait(rsend.at[yy], ys.at[yy])

    loop(0, 4, sent_sums)


def solution(mesh):
    X = mesh.shape["segment"] // 2
    Z = mesh.shape["dp"] // 4

    def on_device(x0, gain, wi, wo, hid, w1, w2):
        x0, wi, wo, hid = x0[0], wi[0], wo[0], hid[0]
        T, W = hid.shape
        N, D = x0.shape
        E = wi.shape[1]
        H = 2 * w1.shape[1]
        half = Z // 2
        B = (96, 256)
        vm = lambda shape, dtype=BF16: pltpu.VMEM(shape, dtype)
        dma = lambda *shape: pltpu.SemaphoreType.DMA(shape)
        scratch = [
            vm((2, D, E)),
            vm((2, E, D)),
            vm((2, 1, D), F32),
            vm((X, T, D)),
            vm((X, T, D)),
            vm((X, T, D)),
            vm((T, D)),
            vm((X, T, W)),
            vm((2 * Z, 2, 64, H)),
            vm((2, 2 * Z, 2, 8, D)),
            vm((X, T, H), F32),
            vm((X, T, H)),
            vm((X, T, D)),
            vm((T, D), F32),
            vm((X, T, D)),
            vm((X, T, D)),
            vm((X, T, H)),
            vm((2, 4, Z) + B),
            vm((4, Z) + B),
            vm((4, Z) + B),
            vm((half, 4) + B),
            vm((half - 1, 4) + B),
            vm((half - 1, 4) + B),
            vm((half - 2, 4) + B),
            vm((4,) + B),
            vm(B, F32),
            vm((4,) + B),
            dma(6 + X),
            dma(2),
            dma(2, 8, CHUNKS),
            dma(2, 8, CHUNKS),
            dma(X),
            dma(X),
            dma(2, 4 * Z),
            dma(2, 4 * Z),
            dma(3),
            dma(3),
            dma(X),
            dma(X),
            dma(X),
            pltpu.SemaphoreType.DMA,
            dma(X),
            dma(X),
            dma(X),
            dma(X),
            dma(4),
            dma(4),
            dma(half, 4),
            dma(half, 4),
            dma(half - 1, 4),
            dma(half - 1, 4),
            dma(4),
            dma(4),
        ]
        any_ = pl.BlockSpec(memory_space=pl.ANY)
        vmem = pl.BlockSpec(memory_space=pltpu.VMEM)
        return pl.pallas_call(
            functools.partial(mega, X, Z),
            out_shape=(
                jax.ShapeDtypeStruct((64, 256), F32),
                jax.ShapeDtypeStruct((8, D), F32),
            ),
            in_specs=[any_] * 7,
            out_specs=(vmem, vmem),
            scratch_shapes=scratch,
            compiler_params=pltpu.CompilerParams(
                collective_id=0, has_side_effects=True, vmem_limit_bytes=62 << 20
            ),
        )(x0, gain, wi, wo, hid, w1, w2)

    placed = (
        P("dp", None, None),
        P("segment", None),
        P("segment", None, None),
        P("segment", None, None),
        P("dp", "segment", None),
        P("dp", "segment"),
        P(("segment", "dp"), None),
    )
    return jax.shard_map(
        on_device,
        mesh=mesh,
        in_specs=placed,
        out_specs=(P("dp", "segment"), P(("segment", "dp"), None)),
        check_vma=False,
    )
```
